32 devices in a mesh: row: 2 (over x), col: 16 (over z, y, core).
Axes of the slice: x: 2, y: 2, z: 4, core: 2. Of those that a mesh axis runs over, the one named last changes fastest.
Arguments:
- adjacency: int32 [2048, 64], P('row', 'col'), may hold values from -2147483648 to 2147483647, as said below
- tile_mask: int32 [16, 16], P('row', 'col'), may hold values from 0 to 1, as said below
- thresholds: int32 [3], replicated, may hold values from 30 to 61
Outputs:
- truss_support: float32 [2048, 2048], P('row', 'col')
- edge_counts: int32 [3], replicated
The draws below stay inside these ranges and needn't reach their ends.
Inputs may be any that keep to these rules, and one draw needn't show every extreme that they name: The graph of adjacency is symmetric with an empty diagonal: bit b of word w of row i equals the bit for row 32 w + b and column i. `tile_mask`: Symmetric.
All inputs are finite; a program needn't handle non-finite values.
Results may differ from the reference program's by a relative error of at most 0.0003.
Values may be sent and summed in bfloat16 or wider, within the bound.
No kernel may reach another device: no remote copies, remote signals or barrier semaphores. Data moves between devices by JAX's collectives and lax.ppermute only.
A program may use at most 64 MiB of HBM per device.

```python
import jax
import jax.numpy as jnp

TILE = 128
ITERS = 3
VERT = 2048


def draw_tile_mask(key, part):
    tiles = VERT // TILE
    base_group = jax.random.randint(jax.random.fold_in(key, 11), (tiles,), 0, 4)
    chooser = jax.random.randint(jax.random.fold_in(key, 12), (tiles,), 0, 3)
    community = jnp.where(chooser == 0, base_group, 0)
    extra_links = jax.random.randint(jax.random.fold_in(key, 13), (tiles, tiles), 0, 10)
    extra_links = jnp.minimum(extra_links, extra_links.T)
    same_group = community[:, None] == community[None, :]
    return jnp.where(same_group | (extra_links < 2), 1, 0).astype(jnp.int32)


def draw_adjacency(key, part):
    tiles = VERT // TILE
    density = jax.random.randint(jax.random.fold_in(key, 21), (tiles, tiles), 30, 400)
    density = (density + density.T) // 2
    level = jnp.repeat(jnp.repeat(density, TILE, axis=0), TILE, axis=1)
    roll = jax.random.randint(jax.random.fold_in(key, 22), (VERT, VERT), 0, 1000)
    vertex = jnp.arange(VERT, dtype=jnp.int32)
    upper = (roll < level) & (vertex[:, None] < vertex[None, :])
    full_graph = (upper | upper.T).astype(jnp.int32)
    shifts = jnp.arange(32, dtype=jnp.int32)
    shifted = jnp.left_shift(full_graph.reshape(VERT, VERT // 32, 32), shifts)
    return jnp.sum(shifted, axis=-1, dtype=jnp.int32).astype(jnp.int32)


def setup_inputs(seed: int = 0) -> dict:
    key_of = jax.random.split(jax.random.key(seed), 4)
    adjacency = draw_adjacency(jax.random.fold_in(key_of[3], 71), 0)
    tile_mask = draw_tile_mask(jax.random.fold_in(key_of[3], 71), 0)
    thresholds = jax.random.randint(key_of[2], (ITERS,), VERT * 15 // 1000, VERT * 30 // 1000 + 1).astype(jnp.int32)
    return dict(adjacency=adjacency, tile_mask=tile_mask, thresholds=thresholds)


def unpack_bits(packed_rows):
    shifts = jnp.arange(32, dtype=jnp.int32)
    flat_bits = jnp.bitwise_and(jnp.right_shift(packed_rows[:, :, None], shifts), 1)
    return flat_bits.reshape(packed_rows.shape[0], packed_rows.shape[1] * 32).astype(jnp.int32)


def reference(adjacency, tile_mask, thresholds):
    flat_bits = unpack_bits(adjacency)
    tile_cover = jnp.repeat(jnp.repeat(tile_mask, TILE, axis=0), TILE, axis=1).astype(jnp.int32)
    surviving = flat_bits * tile_cover
    survived_list = []
    support = jnp.zeros(surviving.shape, jnp.float32)
    for iteration in range(ITERS):
        operand = surviving.astype(jnp.bfloat16)
        wedge_counts = jnp.dot(operand, operand, preferred_element_type=jnp.float32)
        support = wedge_counts * surviving.astype(jnp.float32)
        retained = (support >= thresholds[iteration].astype(jnp.float32)).astype(jnp.int32)
        surviving = surviving * retained
        survived_list.append(jnp.sum(surviving).astype(jnp.int32))
    truss_support = support * surviving.astype(jnp.float32) / thresholds[ITERS - 1].astype(jnp.float32)
    return truss_support, jnp.stack(survived_list).astype(jnp.int32)
```

```python
import functools

import jax
import jax.numpy as jnp
from jax import lax
from jax.experimental import pallas as pl
from jax.experimental.pallas import tpu as pltpu
from jax.sharding import PartitionSpec as P

TILE = 128
ITERS = 3
BLOCK = 512
REPLICATED_LIMIT = 2048
OPERAND = jnp.float8_e4m3fn


def unpack_bits(packed_rows):
    shifts = jnp.arange(32, dtype=jnp.int32)
    flat_bits = jnp.bitwise_and(jnp.right_shift(packed_rows[:, :, None], shifts), 1)
    return flat_bits.reshape(packed_rows.shape[0], packed_rows.shape[1] * 32)


def pack_bits(flat_bits):
    shifts = jnp.arange(32, dtype=jnp.int32)
    grouped = flat_bits.reshape(flat_bits.shape[0], flat_bits.shape[1] // 32, 32)
    return jnp.sum(jnp.left_shift(grouped, shifts), axis=-1, dtype=jnp.int32)


def block_product(packed_rows, matching):
    operand = unpack_bits(packed_rows).astype(jnp.bfloat16)
    return jnp.dot(operand, matching, preferred_element_type=jnp.float32)


def distributed(adjacency, tile_mask, thresholds):
    rows_here = adjacency.shape[0]
    cols_here = adjacency.shape[1] * 32
    flat_bits = unpack_bits(adjacency)
    tile_cover = jnp.broadcast_to(
        tile_mask[:, None, :, None], (tile_mask.shape[0], TILE, tile_mask.shape[1], TILE)
    )
    surviving = flat_bits * tile_cover.reshape(rows_here, cols_here)
    survived_list = []
    support = jnp.zeros((rows_here, cols_here), jnp.float32)
    for iteration in range(ITERS):
        packed_here = pack_bits(surviving)
        column_words = lax.all_gather(packed_here, "row", axis=0, tiled=True)
        column_bits = unpack_bits(column_words)
        lower_panel = column_bits.astype(jnp.bfloat16)
        wedge_counts = block_product(
            lax.all_gather(packed_here, "col", axis=1, tiled=True), lower_panel
        )
        support = wedge_counts * surviving.astype(jnp.float32)
        retained = (support >= thresholds[iteration].astype(jnp.float32)).astype(jnp.int32)
        surviving = surviving * retained
        survived_list.append(jnp.sum(surviving))
    edge_counts = lax.psum(jnp.stack(survived_list), ("row", "col"))
    truss_support = (
        support * surviving.astype(jnp.float32) / thresholds[ITERS - 1].astype(jnp.float32)
    )
    return (truss_support, edge_counts)


def peel_kernel(where_ref, thr_ref, words_ref, out_ref, counts_ref, live_a, live_b):
    n_word_rows, verts = words_ref.shape
    rows_here, cols_here = out_ref.shape
    n_blocks = verts // BLOCK

    def unpack_group(g, carry):
        words = words_ref[pl.ds(pl.multiple_of(g * 8, 8), 8), :]
        shift = lax.broadcasted_iota(jnp.int32, (32, verts), 0)
        for k in range(8):
            row = jnp.broadcast_to(words[k : k + 1, :], (32, verts))
            bits = jnp.bitwise_and(jnp.right_shift(row, shift), 1)
            live_a[pl.ds(pl.multiple_of(g * 256 + k * 32, 32), 32), :] = bits.astype(
                jnp.float32
            ).astype(OPERAND)
        return carry

    lax.fori_loop(0, n_word_rows // 8, unpack_group, 0)

    def sweep(src, dst, thr):
        def outer(bi, acc):
            ri = pl.ds(pl.multiple_of(bi * BLOCK, BLOCK), BLOCK)

            def inner(bj, acc):
                rj = pl.ds(pl.multiple_of(bj * BLOCK, BLOCK), BLOCK)
                wedges = jnp.dot(src[ri, :], src[:, rj], preferred_element_type=jnp.float32)
                old = src[ri, rj].astype(jnp.float32)
                new = jnp.where(wedges >= thr, old, 0.0)
                if dst is not None:
                    dst[ri, rj] = new.astype(OPERAND)
                    dst[rj, ri] = new.T.astype(OPERAND)
                part = jnp.sum(new.reshape(BLOCK // 8, 8, BLOCK), axis=0)
                weight = jnp.where(bi == bj, 1.0, 2.0)
                return acc + part * weight

            return lax.fori_loop(bi, n_blocks, inner, acc)

        acc = lax.fori_loop(0, n_blocks, outer, jnp.zeros((8, BLOCK), jnp.float32))
        return jnp.sum(acc).astype(jnp.int32)

    counts_ref[0] = sweep(live_a, live_b, thr_ref[0].astype(jnp.float32))
    counts_ref[1] = sweep(live_b, live_a, thr_ref[1].astype(jnp.float32))
    last = thr_ref[2].astype(jnp.float32)
    counts_ref[2] = sweep(live_a, None, last)
    ri = pl.ds(pl.multiple_of(where_ref[0] * rows_here, rows_here), rows_here)
    rj = pl.ds(pl.multiple_of(where_ref[1] * cols_here, cols_here), cols_here)
    wedges = jnp.dot(live_a[ri, :], live_a[:, rj], preferred_element_type=jnp.float32)
    old = live_a[ri, rj].astype(jnp.float32)
    out_ref[...] = jnp.where(wedges >= last, wedges * old, 0.0) / last


def gather_words(words, n_rows, n_cols):
    both = lax.all_gather(words, "row", axis=0)
    all_parts = lax.all_gather(both, "col", axis=0)
    n_words = words.shape[0]
    return all_parts.transpose(0, 2, 1, 3).reshape(n_cols * n_words, n_rows * words.shape[1])


def replicated(n_rows, n_cols, adjacency, tile_mask, thresholds):
    rows_here, words_here = adjacency.shape
    cols_here = words_here * 32
    verts = rows_here * n_rows
    cover = jnp.repeat(jnp.repeat(tile_mask.T, TILE, axis=1), TILE // 32, axis=0)
    words = gather_words(adjacency.T * cover, n_rows, n_cols)
    where = jnp.stack([lax.axis_index("row"), lax.axis_index("col")]).astype(jnp.int32)
    return pl.pallas_call(
        peel_kernel,
        in_specs=[
            pl.BlockSpec(memory_space=pltpu.SMEM),
            pl.BlockSpec(memory_space=pltpu.SMEM),
            pl.BlockSpec(memory_space=pltpu.VMEM),
        ],
        out_specs=[
            pl.BlockSpec(memory_space=pltpu.VMEM),
            pl.BlockSpec(memory_space=pltpu.SMEM),
        ],
        out_shape=[
            jax.ShapeDtypeStruct((rows_here, cols_here), jnp.float32),
            jax.ShapeDtypeStruct((ITERS,), jnp.int32),
        ],
        scratch_shapes=[pltpu.VMEM((verts, verts), OPERAND) for _ in range(2)],
        name="peel",
    )(where, thresholds, words)


def local(n_rows, n_cols, adjacency, tile_mask, thresholds):
    verts = adjacency.shape[0] * n_rows
    if verts <= REPLICATED_LIMIT and verts % BLOCK == 0:
        return replicated(n_rows, n_cols, adjacency, tile_mask, thresholds)
    return distributed(adjacency, tile_mask, thresholds)


def solution(mesh):
    in_specs = (P("row", "col"), P("row", "col"), P())
    out_specs = (P("row", "col"), P())
    body = functools.partial(local, mesh.shape["row"], mesh.shape["col"])
    return jax.shard_map(body, mesh=mesh, in_specs=in_specs, out_specs=out_specs, check_vma=False)
```

```python
import functools

import jax
import jax.numpy as jnp
from jax import lax
from jax.experimental import pallas as pl
from jax.experimental.pallas import tpu as pltpu
from jax.sharding import PartitionSpec as P

TILE = 128
ITERS = 3
BLOCK = 512
REPLICATED_LIMIT = 2048
FAR_STRIDE = 4
OPERAND = jnp.float8_e4m3fn


def unpack_bits(packed_rows):
    shifts = jnp.arange(32, dtype=jnp.int32)
    flat_bits = jnp.bitwise_and(jnp.right_shift(packed_rows[:, :, None], shifts), 1)
    return flat_bits.reshape(packed_rows.shape[0], packed_rows.shape[1] * 32)


def pack_bits(flat_bits):
    shifts = jnp.arange(32, dtype=jnp.int32)
    grouped = flat_bits.reshape(flat_bits.shape[0], flat_bits.shape[1] // 32, 32)
    return jnp.sum(jnp.left_shift(grouped, shifts), axis=-1, dtype=jnp.int32)


def block_product(packed_rows, matching):
    operand = unpack_bits(packed_rows).astype(jnp.bfloat16)
    return jnp.dot(operand, matching, preferred_element_type=jnp.float32)


def distributed(adjacency, tile_mask, thresholds):
    rows_here = adjacency.shape[0]
    cols_here = adjacency.shape[1] * 32
    flat_bits = unpack_bits(adjacency)
    tile_cover = jnp.broadcast_to(
        tile_mask[:, None, :, None], (tile_mask.shape[0], TILE, tile_mask.shape[1], TILE)
    )
    surviving = flat_bits * tile_cover.reshape(rows_here, cols_here)
    survived_list = []
    support = jnp.zeros((rows_here, cols_here), jnp.float32)
    for iteration in range(ITERS):
        packed_here = pack_bits(surviving)
        column_words = lax.all_gather(packed_here, "row", axis=0, tiled=True)
        column_bits = unpack_bits(column_words)
        lower_panel = column_bits.astype(jnp.bfloat16)
        wedge_counts = block_product(
            lax.all_gather(packed_here, "col", axis=1, tiled=True), lower_panel
        )
        support = wedge_counts * surviving.astype(jnp.float32)
        retained = (support >= thresholds[iteration].astype(jnp.float32)).astype(jnp.int32)
        surviving = surviving * retained
        survived_list.append(jnp.sum(surviving))
    edge_counts = lax.psum(jnp.stack(survived_list), ("row", "col"))
    truss_support = (
        support * surviving.astype(jnp.float32) / thresholds[ITERS - 1].astype(jnp.float32)
    )
    return (truss_support, edge_counts)


def peel_kernel(where_ref, thr_ref, mine_ref, twin_ref, out_ref, counts_ref, live_a, live_b, wedge_a, wedge_b, *, layout):
    n_rows, n_cols, n_words, fold = layout
    rows_here, cols_here = out_ref.shape
    verts = live_a.shape[0]
    n_blocks = verts // BLOCK
    total = n_blocks * (n_blocks + 1) // 2
    span = rows_here // fold
    row, col = where_ref[0], where_ref[1]
    near = n_cols // FAR_STRIDE

    def unpack_part(part, carry):
        hop, shift = lax.div(part, near), lax.rem(part, near)
        far = lax.rem(lax.div(col, FAR_STRIDE) - shift + near, near)
        row_from = lax.rem(row - lax.div(hop, 2) + n_rows, n_rows)
        col_from = jnp.bitwise_xor(lax.rem(col, FAR_STRIDE), lax.rem(hop, 2) * 2) + far * FAR_STRIDE
        bit = lax.broadcasted_iota(jnp.int32, (32, span), 0)
        for ref, flip in ((mine_ref, 0), (twin_ref, 1)):
            words = ref[part]
            base = jnp.bitwise_xor(col_from, flip) * cols_here
            for k in range(n_words):
                at = pl.ds(pl.multiple_of(base + k * 32, 32), 32)
                for h in range(fold):
                    line = h * n_words + k
                    spread = jnp.broadcast_to(words[line : line + 1, :], (32, span))
                    bits = jnp.bitwise_and(jnp.right_shift(spread, bit), 1)
                    to = pl.ds(pl.multiple_of(row_from * rows_here + h * span, 128), span)
                    live_a[at, to] = bits.astype(jnp.float32).astype(OPERAND)
        return carry

    lax.fori_loop(0, n_rows * n_cols // 2, unpack_part, 0)

    def sweep(src, dst, thr):
        def at(step):
            bi = lax.rem(step, n_blocks)
            bj = lax.rem(bi + lax.div(step, n_blocks), n_blocks)
            return (
                pl.ds(pl.multiple_of(bi * BLOCK, BLOCK), BLOCK),
                pl.ds(pl.multiple_of(bj * BLOCK, BLOCK), BLOCK),
            )

        def product(step, wedges):
            ri, rj = at(step)
            wedges[...] = jnp.dot(src[ri, :], src[:, rj], preferred_element_type=jnp.float32)

        def keep(step, wedges, acc):
            ri, rj = at(step)
            new = jnp.where(wedges[...] >= thr, src[ri, rj].astype(jnp.float32), 0.0)
            if dst is not None:
                narrow = new.astype(OPERAND)
                dst[ri, rj] = narrow
                dst[rj, ri] = narrow.T
            part = jnp.sum(new.reshape(BLOCK // 8, 8, BLOCK), axis=0)
            return acc + part * jnp.where(step < n_blocks, 1.0, 2.0)

        def two_steps(u, acc):
            step = 2 * u
            product(step + 1, wedge_b)
            acc = keep(step, wedge_a, acc)
            product(step + 2, wedge_a)
            return keep(step + 1, wedge_b, acc)

        product(jnp.int32(0), wedge_a)
        turns = (total - 1) // 2
        acc = lax.fori_loop(0, turns, two_steps, jnp.zeros((8, BLOCK), jnp.float32))
        step = jnp.int32(2 * turns)
        if total % 2 == 0:
            product(step + 1, wedge_b)
            acc = keep(step, wedge_a, acc)
            acc = keep(step + 1, wedge_b, acc)
        else:
            acc = keep(step, wedge_a, acc)
        return jnp.sum(acc).astype(jnp.int32)

    counts_ref[0] = sweep(live_a, live_b, thr_ref[0].astype(jnp.float32))
    counts_ref[1] = sweep(live_b, live_a, thr_ref[1].astype(jnp.float32))
    last = thr_ref[2].astype(jnp.float32)
    counts_ref[2] = sweep(live_a, None, last)
    ri = pl.ds(pl.multiple_of(row * rows_here, rows_here), rows_here)
    rj = pl.ds(pl.multiple_of(col * cols_here, cols_here), cols_here)
    wedges = jnp.dot(live_a[ri, :], live_a[:, rj], preferred_element_type=jnp.float32)
    old = live_a[ri, rj].astype(jnp.float32)
    out_ref[...] = jnp.where(wedges >= last, wedges * old, 0.0) / last


def permute(value, n_rows, n_cols, move):
    pairs = [
        (r * n_cols + c, to_r * n_cols + to_c)
        for r in range(n_rows)
        for c in range(n_cols)
        for to_r, to_c in [move(r, c)]
    ]
    return lax.ppermute(value, ("row", "col"), pairs)


def gather_parts(words, n_rows, n_cols):
    near = n_cols // FAR_STRIDE

    def far_move(shift):
        return lambda r, c: (r, c % FAR_STRIDE + (c // FAR_STRIDE + shift) % near * FAR_STRIDE)

    parts = jnp.stack(
        [words] + [permute(words, n_rows, n_cols, far_move(shift)) for shift in range(1, near)]
    )

    def hop_move(hop):
        return lambda r, c: ((r + hop // 2) % n_rows, c ^ (hop % 2 * 2))

    parts = jnp.concatenate(
        [parts] + [permute(parts, n_rows, n_cols, hop_move(hop)) for hop in range(1, 2 * n_rows)]
    )
    return parts, permute(parts, n_rows, n_cols, lambda r, c: (r, c ^ 1))


def replicated(n_rows, n_cols, adjacency, tile_mask, thresholds):
    rows_here, words_here = adjacency.shape
    cols_here = words_here * 32
    verts = rows_here * n_rows
    fold = max(1, 8 // words_here)
    cover = jnp.repeat(jnp.repeat(tile_mask.T, TILE, axis=1), TILE // 32, axis=0)
    words = adjacency.T * cover
    words = jnp.concatenate(jnp.split(words, fold, axis=1), axis=0)
    mine, twin = gather_parts(words, n_rows, n_cols)
    where = jnp.stack([lax.axis_index("row"), lax.axis_index("col")]).astype(jnp.int32)
    return pl.pallas_call(
        functools.partial(peel_kernel, layout=(n_rows, n_cols, words_here, fold)),
        in_specs=[
            pl.BlockSpec(memory_space=pltpu.SMEM),
            pl.BlockSpec(memory_space=pltpu.SMEM),
            pl.BlockSpec(memory_space=pltpu.VMEM),
            pl.BlockSpec(memory_space=pltpu.VMEM),
        ],
        out_specs=[
            pl.BlockSpec(memory_space=pltpu.VMEM),
            pl.BlockSpec(memory_space=pltpu.SMEM),
        ],
        out_shape=[
            jax.ShapeDtypeStruct((rows_here, cols_here), jnp.float32),
            jax.ShapeDtypeStruct((ITERS,), jnp.int32),
        ],
        scratch_shapes=[pltpu.VMEM((verts, verts), OPERAND) for _ in range(2)]
        + [pltpu.VMEM((BLOCK, BLOCK), jnp.float32) for _ in range(2)],
        name="peel",
    )(where, thresholds, mine, twin)


def local(n_rows, n_cols, adjacency, tile_mask, thresholds):
    verts = adjacency.shape[0] * n_rows
    if verts <= REPLICATED_LIMIT and verts % BLOCK == 0 and n_cols % FAR_STRIDE == 0:
        return replicated(n_rows, n_cols, adjacency, tile_mask, thresholds)
    return distributed(adjacency, tile_mask, thresholds)


def solution(mesh):
    in_specs = (P("row", "col"), P("row", "col"), P())
    out_specs = (P("row", "col"), P())
    body = functools.partial(local, mesh.shape["row"], mesh.shape["col"])
    return jax.shard_map(body, mesh=mesh, in_specs=in_specs, out_specs=out_specs, check_vma=False)
```
